512 devices in a mesh: groups: 2 (over y), ctx: 32 (over z, core), tp: 8 (over x).
Axes of the slice: x: 8, y: 2, z: 16, core: 2. Of those that a mesh axis runs over, the one named last changes fastest.
The devices are a block of a 8x8x16 slice.
Arguments:
- q_nope: bfloat16 [4096, 16384], P(('groups', 'ctx'), 'tp'), parts along dimension 0, may hold values from -6 to 6
- q_rope: bfloat16 [4096, 8192], P(('groups', 'ctx'), 'tp'), parts along dimension 0, may hold values from -6 to 6
- c_kv: bfloat16 [4096, 512], P(('groups', 'ctx')), parts along dimension 0, may hold values from -6 to 46.4
- k_rope: bfloat16 [4096, 64], P(('groups', 'ctx')), parts along dimension 0, may hold values from -6 to 6
- positions: int32 [4096], P(('groups', 'ctx')), parts along dimension 0, may hold values from 0 to 2047, as said below
- w_uk: bfloat16 [128, 128, 512], P('tp', 'ctx'), may hold values from -0.5 to 0.5
- w_uv: bfloat16 [128, 512, 128], P('tp', 'ctx'), may hold values from -0.25 to 0.25
- w_out: bfloat16 [16384, 7168], P('tp', 'ctx'), may hold values from -0.125 to 0.125
Outputs:
- attn_proj: bfloat16 [4096, 7168], P(('groups', 'tp'), 'ctx'), parts along dimension 0
The draws below stay inside these ranges and needn't reach their ends.
There are 2 independent parts, one for each index of `groups`. The reference program is written for one: setup_inputs(seed, part) draws one part's arguments, and reference() takes and returns one part's arrays. A program takes and returns all parts, laid end to end along the dimension named above; an argument that names none is the same for every part. Nothing has to cross between parts.
Inputs may be any that keep to these rules, and one draw needn't show every extreme that they name: The positions are the 2048 integers 0 to 2047, each once; every aligned block of 32 rows holds consecutive ascending positions.
All inputs are finite; a program needn't handle non-finite values.
Results may differ from the reference program's by a relative error of at most 0.015.
Values may be sent and summed in bfloat16 or wider, within the bound.
No kernel may reach another device: no remote copies, remote signals or barrier semaphores. Data moves between devices by JAX's collectives and lax.ppermute only.
A program may use at most 64 MiB of HBM per device.

```python
import jax
import jax.numpy as jnp
from jax import lax

D = 7168
HEADS = 128
LAT = 512
ROPE = 64
NOPE = 128
VDIM = 128
TOK_DEV = 64
SEQ = 2048


def draw_c_kv(key, part):
    latent = jnp.clip(jax.random.normal(key, (SEQ, LAT), jnp.float32), -6.0, 6.0)
    return latent.astype(jnp.bfloat16)


def draw_positions(key, part):
    half_len = TOK_DEV // 2
    block_count = SEQ // half_len
    order = jax.random.permutation(jax.random.fold_in(key, 11), block_count)
    grid = order[:, None].astype(jnp.int32) * half_len + jnp.arange(half_len, dtype=jnp.int32)[None, :]
    return grid.reshape(SEQ).astype(jnp.int32)


def block_scale(rng, dims, cuts, low, top_value):
    def one(dim, parts):
        draws = jax.random.uniform(jax.random.fold_in(jax.random.fold_in(rng, 6), dim), (parts,), jnp.float32, low / len(cuts), top_value / len(cuts))
        return jnp.repeat(jnp.exp(draws), dims[dim] // parts).reshape((-1,) + (1,) * (len(dims) - dim - 1))

    loudness = one(*cuts[0])
    for cut in cuts[1:]:
        loudness = loudness * one(*cut)
    return loudness


def scatter_about(key, shape, width, reach, pieces=(), kind=jnp.bfloat16):
    array = jax.random.normal(key, shape, jnp.float32) * width
    if len(pieces) > 0:
        array = block_scale(key, shape, pieces, -0.22, 0.18) * array
    return jnp.clip(array, min=-reach, max=reach).astype(kind)


def setup_inputs(seed: int = 0, part: int = 0) -> dict:
    splits = jax.random.split(jax.random.key(seed), 9)
    own_keys = jax.random.split(jax.random.fold_in(splits[8], part), 9)
    q_nope = scatter_about(own_keys[0], (SEQ, HEADS * NOPE), 1.0, 6.0, ((0, 32), (1, 8)))
    q_rope = scatter_about(own_keys[1], (SEQ, HEADS * ROPE), 1.0, 6.0, ((0, 32), (1, 8)))
    c_kv = draw_c_kv(jax.random.fold_in(jax.random.fold_in(splits[8], part), 71), part)
    k_rope = scatter_about(own_keys[3], (SEQ, ROPE), 1.0, 6.0, ((0, 32),))
    positions = draw_positions(jax.random.fold_in(jax.random.fold_in(splits[8], part), 71), part)
    w_uk = scatter_about(splits[5], (HEADS, NOPE, LAT), NOPE ** -0.5, 0.5, ((0, 8), (1, 32)))
    w_uv = scatter_about(splits[6], (HEADS, LAT, VDIM), LAT ** -0.5, 0.25, ((0, 8), (1, 32)))
    w_out = scatter_about(splits[7], (HEADS * VDIM, D), (HEADS * VDIM // 8) ** -0.5, 0.125, ((0, 8), (1, 32)))
    return {"q_nope": q_nope, "q_rope": q_rope, "c_kv": c_kv, "k_rope": k_rope, "positions": positions, "w_uk": w_uk, "w_uv": w_uv, "w_out": w_out}


def rotate(values, position):
    half_dim = values.shape[-1] // 2
    freqs = 10000.0 ** (-jnp.arange(half_dim, dtype=jnp.float32) / half_dim)
    angles = position.astype(jnp.float32)[..., None] * freqs
    cosine = jnp.cos(angles)
    sine = jnp.sin(angles)
    first_half = values[..., :half_dim].astype(jnp.float32)
    second_half = values[..., half_dim:].astype(jnp.float32)
    return jnp.concatenate([first_half * cosine - second_half * sine, second_half * cosine + first_half * sine], axis=-1)


def reference(q_nope, q_rope, c_kv, k_rope, positions, w_uk, w_uv, w_out):
    softmax_scale = (NOPE + ROPE) ** -0.5
    q_parts = q_nope.reshape(SEQ, HEADS, NOPE).astype(jnp.float32)
    q_lat = jnp.einsum("thn,hnl->htl", q_parts, w_uk.astype(jnp.float32)).astype(jnp.bfloat16)
    q_rot = rotate(q_rope.reshape(SEQ, HEADS, ROPE), positions[:, None]).astype(jnp.bfloat16)
    q_rot = jnp.transpose(q_rot, (1, 0, 2))
    k_rot = rotate(k_rope, positions).astype(jnp.bfloat16)
    key_rows = jnp.concatenate([c_kv, k_rot], axis=1)
    visible = positions[None, :] <= positions[:, None]

    def one_head(operands):
        lat_part, rot_part = operands
        queries = jnp.concatenate([lat_part, rot_part], axis=1)
        scores = jnp.dot(queries, key_rows.T, preferred_element_type=jnp.float32) * softmax_scale
        row_max = jnp.max(jnp.where(visible, scores, -1e30), axis=1)
        weights = jnp.where(visible, jnp.exp(scores - row_max[:, None]), 0.0)
        total = jnp.sum(weights, axis=1)
        mixed = jnp.dot(weights.astype(jnp.bfloat16), c_kv, preferred_element_type=jnp.float32)
        return (mixed / total[:, None]).astype(jnp.bfloat16)

    o_lat = lax.map(one_head, (q_lat, q_rot))
    head_out = jnp.einsum("hsl,hlv->shv", o_lat.astype(jnp.float32), w_uv.astype(jnp.float32))
    head_out = head_out.astype(jnp.bfloat16).reshape(SEQ, HEADS * VDIM)
    return jnp.dot(head_out, w_out, preferred_element_type=jnp.float32).astype(jnp.bfloat16)
```

```python
import functools

import jax
import jax.numpy as jnp
from jax import lax
from jax.experimental import pallas as pl
from jax.experimental.pallas import tpu as pltpu
from jax.sharding import PartitionSpec as P

LANES = 128
DIGIT = 32


def cos_sin(position, half_dim):
    freqs = 10000.0 ** (-jnp.arange(half_dim, dtype=jnp.float32) / half_dim)
    angles = position.astype(jnp.float32)[..., None] * freqs
    return jnp.cos(angles), jnp.sin(angles)


def rotate(values, cosine, sine):
    half_dim = values.shape[-1] // 2
    first_half = values[..., :half_dim].astype(jnp.float32)
    second_half = values[..., half_dim:].astype(jnp.float32)
    return jnp.concatenate(
        [first_half * cosine - second_half * sine, second_half * cosine + first_half * sine],
        axis=-1,
    )


def attend(ranks, toks, lat, tile, scale, qx_ref, qr_ref, qpos_ref, packed, out_ref, wk, keys, wv, q_all, sems):
    groups = qx_ref.shape[0]
    rope_lanes = qr_ref.shape[-1]
    per_group = qx_ref.shape[1]
    wide = lat // rope_lanes

    def copy(i, src, dst):
        c = pltpu.make_async_copy(src, dst, sems.at[i])
        c.start()
        return c

    rows_k, rows_v, rows_r = toks, toks + groups * tile, toks + 2 * groups * tile
    first = copy(0, packed.at[:, rows_k:rows_v, :], wk)
    key_copies = [copy(1, packed.at[:, 0:toks, :], keys.at[:, :, 0:lat])]
    part = toks // wide
    for j in range(wide):
        key_copies.append(
            copy(
                3 + j,
                packed.at[:, rows_r : rows_r + part, j * rope_lanes : (j + 1) * rope_lanes],
                keys.at[:, j * part : (j + 1) * part, lat : lat + rope_lanes],
            )
        )
    last = copy(2, packed.at[:, rows_v:rows_r, :], wv)
    first.wait()
    for g in range(groups):
        w = wk[:, g * tile : (g + 1) * tile, :].reshape(ranks * tile, lat)
        q_lat = jnp.dot(qx_ref[g], w, preferred_element_type=jnp.float32)
        q_all[g, :, 0:lat] = q_lat.astype(jnp.bfloat16)
        q_all[g, :, lat:] = qr_ref[g]
    for c in key_copies:
        c.wait()
    all_keys = keys[...].reshape(ranks * toks, lat + rope_lanes)
    lane = lax.broadcasted_iota(jnp.int32, (8, rope_lanes), 1)
    half = rope_lanes // 2
    pick = jnp.where(lane == half, float(DIGIT), jnp.where(lane == half + 1, 1.0, 0.0))
    key_pos = lax.dot_general(
        pick.astype(jnp.bfloat16),
        all_keys[:, lat:],
        (((1,), (1,)), ((), ())),
        preferred_element_type=jnp.float32,
    )[0:1]
    visible = key_pos <= qpos_ref[...]
    last.wait()
    factor = scale * 1.4426950408889634
    head_dim = lat // (per_group // toks)
    for g in range(groups):
        scores = lax.dot_general(
            q_all[g], all_keys, (((1,), (1,)), ((), ())), preferred_element_type=jnp.float32
        )
        scores = jnp.where(visible, scores, -1e30)
        top = jnp.max(scores, axis=1, keepdims=True)
        weights = jnp.exp2((scores - top) * factor)
        total = jnp.sum(weights, axis=1, keepdims=True)
        mixed = jnp.dot(
            weights.astype(jnp.bfloat16), all_keys[:, :lat], preferred_element_type=jnp.float32
        )
        o_lat = (mixed / total).astype(jnp.bfloat16)
        w = wv[:, g * tile : (g + 1) * tile, :].reshape(ranks * tile, lat)
        head_out = jnp.dot(o_lat, w, preferred_element_type=jnp.float32).astype(jnp.bfloat16)
        for h in range(per_group // toks):
            at = g * lat + h * head_dim
            out_ref[:, at : at + head_dim] = head_out[
                h * toks : (h + 1) * toks, h * head_dim : (h + 1) * head_dim
            ]


def on_device(q_nope, q_rope, c_kv, k_rope, positions, w_uk, w_uv, w_out):
    toks, lat = c_kv.shape
    heads, tile_rows, _ = w_uk.shape
    ranks = lax.axis_size("ctx")
    nope = tile_rows * ranks
    rope = k_rope.shape[1]
    v_dim = w_uv.shape[2]
    v_rows = w_uv.shape[1]
    scale = (nope + rope) ** (-0.5)
    group = lat // v_dim
    groups = heads // group
    tile = group * tile_rows
    assert tile == v_rows and group * nope == lat
    cosine, sine = cos_sin(positions, rope // 2)

    k_rot = rotate(k_rope, cosine, sine).astype(jnp.bfloat16)
    digits = jnp.stack([positions // DIGIT, positions % DIGIT], axis=1).astype(jnp.bfloat16)
    rot_part = jnp.concatenate(
        [k_rot, digits, jnp.zeros((toks, LANES - rope - 2), jnp.bfloat16)], axis=1
    )
    wide = lat // LANES
    rot_part = rot_part.reshape(wide, toks // wide, LANES).transpose(1, 0, 2).reshape(-1, lat)
    v_part = w_uv.reshape(groups, group, v_rows, v_dim).transpose(0, 2, 1, 3).reshape(-1, lat)
    own = jnp.concatenate([c_kv, w_uk.reshape(-1, lat), v_part, rot_part], axis=0)
    packed = lax.all_gather(own, "ctx", axis=0)

    row = lax.broadcasted_iota(jnp.int32, (lat, lat), 0)
    col = lax.broadcasted_iota(jnp.int32, (lat, lat), 1)
    target = (row % nope) // tile_rows * tile + (row // nope) * tile_rows + row % tile_rows
    order = (col == target).astype(jnp.bfloat16)
    q_groups = q_nope.reshape(toks, groups, lat).transpose(1, 0, 2)
    head_of = lax.broadcasted_iota(jnp.int32, (1, group, 1, lat), 3) // nope
    head = lax.broadcasted_iota(jnp.int32, (1, group, 1, lat), 1)
    q_masked = jnp.where(head_of == head, q_groups[:, None], jnp.bfloat16(0))
    qx = jnp.dot(
        q_masked.reshape(heads * toks, lat), order, preferred_element_type=jnp.float32
    ).astype(jnp.bfloat16)
    qx = qx.reshape(groups, group * toks, lat)
    q_rot = rotate(
        q_rope.reshape(toks, heads, rope), cosine[:, None], sine[:, None]
    ).astype(jnp.bfloat16)
    q_rot = jnp.pad(q_rot.transpose(1, 0, 2), ((0, 0), (0, 0), (0, LANES - rope)))
    q_rot = q_rot.reshape(groups, group * toks, LANES)
    q_pos = jnp.tile(positions.astype(jnp.float32), group)[:, None]

    vmem = pl.BlockSpec(memory_space=pltpu.VMEM)
    rows_out = pl.pallas_call(
        functools.partial(attend, ranks, toks, lat, tile, scale),
        out_shape=jax.ShapeDtypeStruct((toks, heads * v_dim), jnp.bfloat16),
        in_specs=[vmem, vmem, vmem, pl.BlockSpec(memory_space=pl.ANY)],
        out_specs=vmem,
        scratch_shapes=[
            pltpu.VMEM((ranks, groups * tile, lat), jnp.bfloat16),
            pltpu.VMEM((ranks, toks, lat + LANES), jnp.bfloat16),
            pltpu.VMEM((ranks, groups * tile, lat), jnp.bfloat16),
            pltpu.VMEM((groups, group * toks, lat + LANES), jnp.bfloat16),
            pltpu.SemaphoreType.DMA((3 + wide,)),
        ],
    )(qx, q_rot, q_pos, packed)

    partial_value = jnp.dot(
        lax.all_gather(rows_out, "ctx", axis=0, tiled=True),
        w_out,
        preferred_element_type=jnp.float32,
    ).astype(jnp.bfloat16)
    blocks = partial_value.reshape(lax.axis_size("tp"), -1, partial_value.shape[1])
    arrived = lax.all_to_all(blocks, "tp", split_axis=0, concat_axis=0, tiled=True)
    return arrived.astype(jnp.float32).sum(axis=0).astype(jnp.bfloat16)


def solution(mesh):
    in_specs = (
        P(("groups", "ctx"), "tp"),
        P(("groups", "ctx"), "tp"),
        P(("groups", "ctx"), None),
        P(("groups", "ctx"), None),
        P(("groups", "ctx")),
        P("tp", "ctx", None),
        P("tp", "ctx", None),
        P("tp", "ctx"),
    )
    out_specs = P(("groups", "tp"), "ctx")
    return jax.shard_map(
        on_device, mesh=mesh, in_specs=in_specs, out_specs=out_specs, check_vma=False
    )
```

```python
import functools

import jax
import jax.numpy as jnp
from jax import lax
from jax.experimental import pallas as pl
from jax.experimental.pallas import tpu as pltpu
from jax.sharding import PartitionSpec as P

LANES = 128
DIGIT = 32
CORES = 2


def cos_sin(position, half_dim):
    freqs = 10000.0 ** (-jnp.arange(half_dim, dtype=jnp.float32) / half_dim)
    angles = position.astype(jnp.float32)[..., None] * freqs
    return jnp.cos(angles), jnp.sin(angles)


def rotate(values, cosine, sine):
    half_dim = values.shape[-1] // 2
    first_half = values[..., :half_dim].astype(jnp.float32)
    second_half = values[..., half_dim:].astype(jnp.float32)
    return jnp.concatenate(
        [first_half * cosine - second_half * sine, second_half * cosine + first_half * sine],
        axis=-1,
    )


def attend(chips, toks, lat, scale, block, core_ref, q_ref, wv_ref, packed, out_ref, keys, sems):
    wide = lat // LANES
    part = toks // wide
    copies = [pltpu.make_async_copy(packed.at[:, :, 0:toks, :], keys.at[:, :, :, 0:lat], sems.at[0])]
    for j in range(wide):
        copies.append(
            pltpu.make_async_copy(
                packed.at[:, :, toks : toks + part, j * LANES : (j + 1) * LANES],
                keys.at[:, :, j * part : (j + 1) * part, lat : lat + LANES],
                sems.at[1 + j],
            )
        )
    for c in copies:
        c.start()
    for c in copies:
        c.wait()
    all_keys = keys[...].reshape(chips * CORES * toks, lat + LANES)
    half = LANES // 2
    lane = lax.broadcasted_iota(jnp.int32, (LANES, LANES), 1)
    pick = jnp.where(lane == half, float(DIGIT), jnp.where(lane == half + 1, 1.0, 0.0))
    pick = pick.astype(jnp.bfloat16)
    nt = (((1,), (1,)), ((), ()))
    key_pos = lax.dot_general(pick[0:8], all_keys[:, lat:], nt, preferred_element_type=jnp.float32)[0:1]
    own = keys[:, pl.ds(core_ref[0], 1), :, lat : lat + LANES].reshape(chips * toks, LANES)
    q_pos = lax.dot_general(own, pick, nt, preferred_element_type=jnp.float32)[:, 0:1]
    factor = scale * 1.4426950408889634
    for b in range(chips * toks // block):
        rows = slice(b * block, (b + 1) * block)
        scores = lax.dot_general(q_ref[rows, :], all_keys, nt, preferred_element_type=jnp.float32)
        scores = jnp.where(key_pos <= q_pos[rows], scores, -1e30)
        top = jnp.max(scores, axis=1, keepdims=True)
        weights = jnp.exp2((scores - top) * factor)
        total = jnp.sum(weights, axis=1, keepdims=True)
        mixed = jnp.dot(
            weights.astype(jnp.bfloat16), all_keys[:, :lat], preferred_element_type=jnp.float32
        )
        o_lat = (mixed / total).astype(jnp.bfloat16)
        out_ref[rows, :] = jnp.dot(
            o_lat, wv_ref[...], preferred_element_type=jnp.float32
        ).astype(jnp.bfloat16)


def project(chips, planes, toks, steps, gathered, weights, out_ref, heads_buf, w_buf, sems):
    each = chips // steps
    pairs = heads_buf.shape[2] // (CORES * toks)
    v_dim = heads_buf.shape[3]
    copies = []
    for s in range(steps):
        zs = slice(s * each, (s + 1) * each)
        group = [
            pltpu.make_async_copy(
                weights.at[:, :, s * each * v_dim : (s + 1) * each * v_dim], w_buf.at[s], sems.at[s, 0]
            )
        ]
        for pair in range(pairs):
            for k in range(CORES):
                at = (pair * CORES + k) * toks
                group.append(
                    pltpu.make_async_copy(
                        gathered.at[zs, k, :, pair * toks : (pair + 1) * toks, :],
                        heads_buf.at[zs, :, at : at + toks, :],
                        sems.at[s, 1 + pair * CORES + k],
                    )
                )
        copies.append(group)
    for group in copies:
        for c in group:
            c.start()
    total = None
    for s in range(steps):
        for c in copies[s]:
            c.wait()
        for i in range(each):
            z = s * each + i
            rows = jnp.concatenate([heads_buf[z, x] for x in range(planes)], axis=1)
            w = jnp.concatenate(
                [w_buf[s, x, :, i * v_dim : (i + 1) * v_dim] for x in range(planes)], axis=1
            )
            added = lax.dot_general(
                w, rows, (((1,), (1,)), ((), ())), preferred_element_type=jnp.float32
            )
            total = added if total is None else total + added
    out_ref[...] = total.astype(jnp.bfloat16)


def on_device(q_nope, q_rope, c_kv, k_rope, positions, w_uk, w_uv, w_out):
    toks, lat = c_kv.shape
    heads, tile_rows, _ = w_uk.shape
    ranks = lax.axis_size("ctx")
    planes = lax.axis_size("tp")
    chips = ranks // CORES
    assert heads == chips
    nope = tile_rows * ranks
    rope = k_rope.shape[1]
    v_rows, v_dim = w_uv.shape[1:]
    scale = (nope + rope) ** (-0.5)
    same_core = [[z * CORES + k for z in range(chips)] for k in range(CORES)]
    one_chip = [[z * CORES + k for k in range(CORES)] for z in range(chips)]
    cosine, sine = cos_sin(positions, rope // 2)

    k_rot = rotate(k_rope, cosine, sine).astype(jnp.bfloat16)
    digits = jnp.stack([positions // DIGIT, positions % DIGIT], axis=1).astype(jnp.bfloat16)
    rot_part = jnp.concatenate(
        [k_rot, digits, jnp.zeros((toks, LANES - rope - 2), jnp.bfloat16)], axis=1
    )
    wide = lat // LANES
    rot_part = rot_part.reshape(wide, toks // wide, LANES).transpose(1, 0, 2).reshape(-1, lat)
    packed = lax.all_gather(jnp.concatenate([c_kv, rot_part], axis=0), "ctx", axis=0)
    packed = packed.reshape(chips, CORES, toks + toks // wide, lat)

    q_parts = q_nope.reshape(toks, heads, nope).transpose(1, 0, 2)
    q_rot = rotate(q_rope.reshape(toks, heads, rope), cosine[:, None], sine[:, None])
    q_rot = q_rot.astype(jnp.bfloat16).transpose(1, 0, 2)
    q_rot = jnp.concatenate([q_rot[:, : toks // 2], q_rot[:, toks // 2 :]], axis=2)
    k_rows = tile_rows * wide
    sent = jnp.concatenate([q_parts, q_rot, w_uk.reshape(heads, k_rows, LANES), w_uv], axis=1)
    came = lax.all_to_all(
        sent, "ctx", split_axis=0, concat_axis=0, tiled=True, axis_index_groups=same_core
    )
    cut = toks + toks // 2
    q_parts = came[:, :toks].reshape(chips * toks, nope)
    q_rot = came[:, toks:cut]
    q_rot = jnp.concatenate([q_rot[:, :, :rope], q_rot[:, :, rope:]], axis=1).reshape(-1, rope)
    both = lax.all_to_all(
        jnp.broadcast_to(came[None, :, cut:], (CORES, chips, k_rows + v_rows, LANES)),
        "ctx",
        split_axis=0,
        concat_axis=0,
        tiled=True,
        axis_index_groups=one_chip,
    ).transpose(1, 0, 2, 3)
    up_key = both[:, :, :k_rows].reshape(nope, lat)
    up_value = both[:, :, k_rows:].reshape(lat, v_dim)
    q_lat = jnp.dot(q_parts, up_key, preferred_element_type=jnp.float32).astype(jnp.bfloat16)
    queries = jnp.concatenate(
        [q_lat, q_rot, jnp.zeros((chips * toks, LANES - rope), jnp.bfloat16)], axis=1
    )

    plane = lax.axis_index("tp")
    own_w = w_out.T
    right = [(i, (i + 1) % planes) for i in range(planes)]
    left = [(i, (i - 1) % planes) for i in range(planes)]
    all_w = jnp.zeros((planes, *own_w.shape), jnp.bfloat16)

    def placed(stack, block, shift):
        return lax.dynamic_update_slice(stack, block[None], ((plane + shift) % planes, 0, 0))

    def spread(stack, lower, upper, first, until):
        for s in range(first, until):
            lower = lax.ppermute(lower, "tp", right)
            stack = placed(stack, lower, planes - s)
            if 2 * s < planes:
                upper = lax.ppermute(upper, "tp", left)
                stack = placed(stack, upper, s)
        return stack, lower, upper

    all_w = placed(all_w, own_w, 0)
    early = planes // 4
    all_w, lower, upper = spread(all_w, own_w, own_w, 1, 1 + early)

    vmem = pl.BlockSpec(memory_space=pltpu.VMEM)
    smem = pl.BlockSpec(memory_space=pltpu.SMEM)
    hbm = pl.BlockSpec(memory_space=pl.ANY)
    core = (lax.axis_index("ctx") % CORES).astype(jnp.int32).reshape(1)
    block = min(256, chips * toks)
    head_out = pl.pallas_call(
        functools.partial(attend, chips, toks, lat, scale, block),
        out_shape=jax.ShapeDtypeStruct((chips * toks, v_dim), jnp.bfloat16),
        in_specs=[smem, vmem, vmem, hbm],
        out_specs=vmem,
        scratch_shapes=[
            pltpu.VMEM((chips, CORES, toks, lat + LANES), jnp.bfloat16),
            pltpu.SemaphoreType.DMA((1 + wide,)),
        ],
    )(core, queries, up_value, packed)

    head_out, all_w, lower, upper = lax.optimization_barrier((head_out, all_w, lower, upper))
    by_plane = lax.all_to_all(
        head_out.reshape(planes, -1, v_dim), "tp", split_axis=0, concat_axis=0, tiled=True
    )
    gathered = lax.all_gather(by_plane.reshape(-1, v_dim), "ctx", axis=0)
    gathered = gathered.reshape(chips, CORES, planes, -1, v_dim)
    all_w, _, _ = spread(all_w, lower, upper, 1 + early, planes // 2 + 1)

    out_toks = gathered.shape[3] * CORES
    columns = w_out.shape[1]
    steps = 4
    out = pl.pallas_call(
        functools.partial(project, chips, planes, toks, steps),
        out_shape=jax.ShapeDtypeStruct((columns, out_toks), jnp.bfloat16),
        in_specs=[hbm, hbm],
        out_specs=vmem,
        scratch_shapes=[
            pltpu.VMEM((chips, planes, out_toks, v_dim), jnp.bfloat16),
            pltpu.VMEM((steps, planes, columns, chips // steps * v_dim), jnp.bfloat16),
            pltpu.SemaphoreType.DMA((steps, 1 + out_toks // toks)),
        ],
    )(gathered, all_w)
    return out.T


def solution(mesh):
    in_specs = (
        P(("groups", "ctx"), "tp"),
        P(("groups", "ctx"), "tp"),
        P(("groups", "ctx"), None),
        P(("groups", "ctx"), None),
        P(("groups", "ctx")),
        P("tp", "ctx", None),
        P("tp", "ctx", None),
        P("tp", "ctx"),
    )
    out_specs = P(("groups", "tp"), "ctx")
    return jax.shard_map(
        on_device, mesh=mesh, in_specs=in_specs, out_specs=out_specs, check_vma=False
    )
```

```python
import functools

import jax
import jax.numpy as jnp
from jax import lax
from jax.experimental import pallas as pl
from jax.experimental.pallas import tpu as pltpu
from jax.sharding import PartitionSpec as P


LANES = 128
DIGIT = 32
CORES = 2


def cos_sin(position, half_dim):
    freqs = 10000.0 ** (-jnp.arange(half_dim, dtype=jnp.float32) / half_dim)
    angles = position.astype(jnp.float32)[..., None] * freqs
    return jnp.cos(angles), jnp.sin(angles)


def rotate(values, cosine, sine):
    half_dim = values.shape[-1] // 2
    first_half = values[..., :half_dim].astype(jnp.float32)
    second_half = values[..., half_dim:].astype(jnp.float32)
    return jnp.concatenate(
        [first_half * cosine - second_half * sine, second_half * cosine + first_half * sine],
        axis=-1,
    )


def attend(chips, planes, toks, lat, scale, block, q_ref, wv_ref, own_ref, other_ref, out_ref, pos_buf):
    share = toks // planes
    half = LANES // 2
    lane = lax.broadcasted_iota(jnp.int32, (LANES, LANES), 1)
    pick = jnp.where(lane == half, float(DIGIT), jnp.where(lane == half + 1, 1.0, 0.0))
    pick = pick.astype(jnp.bfloat16)
    nt = (((1,), (1,)), ((), ()))
    all_keys = jnp.concatenate([own_ref[...], other_ref[...]], axis=0)
    key_pos = lax.dot_general(pick[0:8], all_keys[:, lat:], nt, preferred_element_type=jnp.float32)[0:1]
    own_pos = lax.dot_general(own_ref[:, lat:], pick, nt, preferred_element_type=jnp.float32)
    own_pos = own_pos.reshape(planes, chips, share, LANES)
    for x in range(planes):
        pos_buf[:, x] = own_pos[x]
    q_pos = pos_buf[...].reshape(chips * toks, LANES)[:, 0:1]
    factor = scale * 1.4426950408889634
    for b in range(chips * toks // block):
        rows = slice(b * block, (b + 1) * block)
        scores = lax.dot_general(q_ref[rows, :], all_keys, nt, preferred_element_type=jnp.float32)
        scores = jnp.where(key_pos <= q_pos[rows], scores, -1e30)
        top = jnp.max(scores, axis=1, keepdims=True)
        weights = jnp.exp2((scores - top) * factor)
        total = jnp.sum(weights, axis=1, keepdims=True)
        mixed = jnp.dot(
            weights.astype(jnp.bfloat16), all_keys[:, :lat], preferred_element_type=jnp.float32
        )
        o_lat = (mixed / total).astype(jnp.bfloat16)
        out_ref[rows, :] = jnp.dot(
            o_lat, wv_ref[...], preferred_element_type=jnp.float32
        ).astype(jnp.bfloat16)


def project(chips, planes, toks, steps, gathered, weights, out_ref, heads_buf, w_buf, sems):
    each = chips // steps
    pairs = heads_buf.shape[2] // (CORES * toks)
    v_dim = heads_buf.shape[3]
    copies = []
    for s in range(steps):
        zs = slice(s * each, (s + 1) * each)
        group = [
            pltpu.make_async_copy(
                weights.at[:, :, s * each * v_dim : (s + 1) * each * v_dim], w_buf.at[s], sems.at[s, 0]
            )
        ]
        for pair in range(pairs):
            for k in range(CORES):
                at = (pair * CORES + k) * toks
                group.append(
                    pltpu.make_async_copy(
                        gathered.at[zs, k, :, pair * toks : (pair + 1) * toks, :],
                        heads_buf.at[zs, :, at : at + toks, :],
                        sems.at[s, 1 + pair * CORES + k],
                    )
                )
        copies.append(group)
    for group in copies:
        for c in group:
            c.start()
    total = None
    for s in range(steps):
        for c in copies[s]:
            c.wait()
        for i in range(each):
            z = s * each + i
            rows = jnp.concatenate([heads_buf[z, x] for x in range(planes)], axis=1)
            w = jnp.concatenate(
                [w_buf[s, x, :, i * v_dim : (i + 1) * v_dim] for x in range(planes)], axis=1
            )
            added = lax.dot_general(
                w, rows, (((1,), (1,)), ((), ())), preferred_element_type=jnp.float32
            )
            total = added if total is None else total + added
    out_ref[...] = total.astype(jnp.bfloat16)


def on_device(q_nope, q_rope, c_kv, k_rope, positions, w_uk, w_uv, w_out):
    toks, lat = c_kv.shape
    heads, tile_rows, _ = w_uk.shape
    ranks = lax.axis_size("ctx")
    planes = lax.axis_size("tp")
    chips = ranks // CORES
    assert heads == chips
    nope = tile_rows * ranks
    rope = k_rope.shape[1]
    v_rows, v_dim = w_uv.shape[1:]
    scale = (nope + rope) ** (-0.5)
    same_core = [[z * CORES + k for z in range(chips)] for k in range(CORES)]
    one_chip = [[z * CORES + k for k in range(CORES)] for z in range(chips)]

    plane = lax.axis_index("tp")
    share = toks // planes

    def cut_share(a):
        return lax.dynamic_slice_in_dim(a, plane * share, share, 0)

    own_pos = cut_share(positions)
    k_rot = rotate(cut_share(k_rope), *cos_sin(own_pos, rope // 2)).astype(jnp.bfloat16)
    digits = jnp.stack([own_pos // DIGIT, own_pos % DIGIT], axis=1).astype(jnp.bfloat16)
    zeros = jnp.zeros((share, LANES - rope - 2), jnp.bfloat16)
    own_keys = jnp.concatenate([cut_share(c_kv), k_rot, digits, zeros], axis=1)
    own_keys = jnp.broadcast_to(own_keys, (chips, *own_keys.shape))
    own_keys = lax.all_to_all(
        own_keys, "ctx", split_axis=0, concat_axis=0, tiled=True, axis_index_groups=same_core
    )
    own_keys = lax.all_gather(own_keys.reshape(chips * share, -1), "tp", axis=0, tiled=True)
    swap = [(r, r // CORES * CORES + (r + 1) % CORES) for r in range(ranks)]
    other_keys = lax.ppermute(own_keys, "ctx", swap)

    cosine, sine = cos_sin(positions, rope // 2)
    q_parts = q_nope.reshape(toks, heads, nope).transpose(1, 0, 2)
    q_rot = rotate(q_rope.reshape(toks, heads, rope), cosine[:, None], sine[:, None])
    q_rot = q_rot.astype(jnp.bfloat16).transpose(1, 0, 2)
    q_rot = jnp.concatenate([q_rot[:, : toks // 2], q_rot[:, toks // 2 :]], axis=2)
    k_rows = tile_rows * lat // LANES
    sent = jnp.concatenate([q_parts, q_rot, w_uk.reshape(heads, k_rows, LANES), w_uv], axis=1)
    came = lax.all_to_all(
        sent, "ctx", split_axis=0, concat_axis=0, tiled=True, axis_index_groups=same_core
    )
    cut = toks + toks // 2
    q_parts = came[:, :toks].reshape(chips * toks, nope)
    q_rot = came[:, toks:cut]
    q_rot = jnp.concatenate([q_rot[:, :, :rope], q_rot[:, :, rope:]], axis=1).reshape(-1, rope)
    both = lax.all_to_all(
        jnp.broadcast_to(came[None, :, cut:], (CORES, chips, k_rows + v_rows, LANES)),
        "ctx",
        split_axis=0,
        concat_axis=0,
        tiled=True,
        axis_index_groups=one_chip,
    ).transpose(1, 0, 2, 3)
    up_key = both[:, :, :k_rows].reshape(nope, lat)
    up_value = both[:, :, k_rows:].reshape(lat, v_dim)
    q_lat = jnp.dot(q_parts, up_key, preferred_element_type=jnp.float32).astype(jnp.bfloat16)
    queries = jnp.concatenate(
        [q_lat, q_rot, jnp.zeros((chips * toks, LANES - rope), jnp.bfloat16)], axis=1
    )

    own_w = w_out.T
    right = [(i, (i + 1) % planes) for i in range(planes)]
    left = [(i, (i - 1) % planes) for i in range(planes)]
    all_w = jnp.zeros((planes, *own_w.shape), jnp.bfloat16)

    def placed(stack, block, shift):
        return lax.dynamic_update_slice(stack, block[None], ((plane + shift) % planes, 0, 0))

    lower = lax.ppermute(own_w, "tp", right)
    all_w = placed(placed(all_w, own_w, 0), lower, planes - 1)
    upper = own_w

    vmem = pl.BlockSpec(memory_space=pltpu.VMEM)
    hbm = pl.BlockSpec(memory_space=pl.ANY)
    block = min(256, chips * toks)
    head_out = pl.pallas_call(
        functools.partial(attend, chips, planes, toks, lat, scale, block),
        out_shape=jax.ShapeDtypeStruct((chips * toks, v_dim), jnp.bfloat16),
        in_specs=[vmem, vmem, vmem, vmem],
        out_specs=vmem,
        scratch_shapes=[pltpu.VMEM((chips, planes, share, LANES), jnp.float32)],
    )(queries, up_value, own_keys, other_keys)

    head_out, all_w, lower, upper = lax.optimization_barrier((head_out, all_w, lower, upper))
    by_plane = lax.all_to_all(
        head_out.reshape(planes, -1, v_dim), "tp", split_axis=0, concat_axis=0, tiled=True
    )
    gathered = lax.all_gather(by_plane.reshape(-1, v_dim), "ctx", axis=0)
    gathered = gathered.reshape(chips, CORES, planes, -1, v_dim)
    for s in range(1, planes // 2):
        lower = lax.ppermute(lower, "tp", right)
        upper = lax.ppermute(upper, "tp", left)
        all_w = placed(placed(all_w, lower, planes - 1 - s), upper, s)

    out_toks = gathered.shape[3] * CORES
    columns = w_out.shape[1]
    steps = 4
    out = pl.pallas_call(
        functools.partial(project, chips, planes, toks, steps),
        out_shape=jax.ShapeDtypeStruct((columns, out_toks), jnp.bfloat16),
        in_specs=[hbm, hbm],
        out_specs=vmem,
        scratch_shapes=[
            pltpu.VMEM((chips, planes, out_toks, v_dim), jnp.bfloat16),
            pltpu.VMEM((steps, planes, columns, chips // steps * v_dim), jnp.bfloat16),
            pltpu.SemaphoreType.DMA((steps, 1 + out_toks // toks)),
        ],
    )(gathered, all_w)
    return out.T


def solution(mesh):
    in_specs = (
        P(("groups", "ctx"), "tp"),
        P(("groups", "ctx"), "tp"),
        P(("groups", "ctx"), None),
        P(("groups", "ctx"), None),
        P(("groups", "ctx")),
        P("tp", "ctx", None),
        P("tp", "ctx", None),
        P("tp", "ctx"),
    )
    out_specs = P(("groups", "tp"), "ctx")

    return jax.shard_map(on_device, mesh=mesh, in_specs=in_specs, out_specs=out_specs, check_vma=False)
```

```python
import functools

import jax
import jax.numpy as jnp
from jax import lax
from jax.experimental import pallas as pl
from jax.experimental.pallas import tpu as pltpu
from jax.sharding import PartitionSpec as P


LANES = 128
DIGIT = 32
CORES = 2


def cos_sin(position, half_dim):
    freqs = 10000.0 ** (-jnp.arange(half_dim, dtype=jnp.float32) / half_dim)
    angles = position.astype(jnp.float32)[..., None] * freqs
    return jnp.cos(angles), jnp.sin(angles)


def rotate(values, cosine, sine):
    half_dim = values.shape[-1] // 2
    first_half = values[..., :half_dim].astype(jnp.float32)
    second_half = values[..., half_dim:].astype(jnp.float32)
    return jnp.concatenate(
        [first_half * cosine - second_half * sine, second_half * cosine + first_half * sine],
        axis=-1,
    )


def attend(chips, planes, toks, lat, scale, block, q_ref, wv_ref, own_ref, other_ref, out_ref, pos_buf):
    share = toks // planes
    half = LANES // 2
    lane = lax.broadcasted_iota(jnp.int32, (LANES, LANES), 1)
    pick = jnp.where(lane == half, float(DIGIT), jnp.where(lane == half + 1, 1.0, 0.0))
    pick = pick.astype(jnp.bfloat16)
    nt = (((1,), (1,)), ((), ()))
    all_keys = jnp.concatenate([own_ref[...], other_ref[...]], axis=0)
    key_pos = lax.dot_general(pick[0:8], all_keys[:, lat:], nt, preferred_element_type=jnp.float32)[0:1]
    own_pos = lax.dot_general(own_ref[:, lat:], pick, nt, preferred_element_type=jnp.float32)
    own_pos = own_pos.reshape(planes, chips, share, LANES)
    for x in range(planes):
        pos_buf[:, x] = own_pos[x]
    q_pos = pos_buf[...].reshape(chips * toks, LANES)[:, 0:1]
    factor = scale * 1.4426950408889634
    for b in range(chips * toks // block):
        rows = slice(b * block, (b + 1) * block)
        scores = lax.dot_general(q_ref[rows, :], all_keys, nt, preferred_element_type=jnp.float32)
        scores = jnp.where(key_pos <= q_pos[rows], scores, -1e30)
        top = jnp.max(scores, axis=1, keepdims=True)
        weights = jnp.exp2((scores - top) * factor)
        total = jnp.sum(weights, axis=1, keepdims=True)
        mixed = jnp.dot(
            weights.astype(jnp.bfloat16), all_keys[:, :lat], preferred_element_type=jnp.float32
        )
        o_lat = (mixed / total).astype(jnp.bfloat16)
        out_ref[rows, :] = jnp.dot(
            o_lat, wv_ref[...], preferred_element_type=jnp.float32
        ).astype(jnp.bfloat16)


def project(chips, planes, toks, steps, gathered, weights, out_ref, heads_buf, w_buf, sems):
    each = chips // steps
    pairs = heads_buf.shape[2] // (CORES * toks)
    v_dim = heads_buf.shape[3]
    copies = []
    for s in range(steps):
        zs = slice(s * each, (s + 1) * each)
        group = [
            pltpu.make_async_copy(
                weights.at[:, :, s * each * v_dim : (s + 1) * each * v_dim], w_buf.at[s], sems.at[s, 0]
            )
        ]
        for pair in range(pairs):
            for k in range(CORES):
                at = (pair * CORES + k) * toks
                group.append(
                    pltpu.make_async_copy(
                        gathered.at[zs, k, :, pair * toks : (pair + 1) * toks, :],
                        heads_buf.at[zs, :, at : at + toks, :],
                        sems.at[s, 1 + pair * CORES + k],
                    )
                )
        copies.append(group)
    for group in copies:
        for c in group:
            c.start()
    total = None
    for s in range(steps):
        for c in copies[s]:
            c.wait()
        for i in range(each):
            z = s * each + i
            rows = jnp.concatenate([heads_buf[z, x] for x in range(planes)], axis=1)
            w = jnp.concatenate(
                [w_buf[s, x, :, i * v_dim : (i + 1) * v_dim] for x in range(planes)], axis=1
            )
            added = lax.dot_general(
                w, rows, (((1,), (1,)), ((), ())), preferred_element_type=jnp.float32
            )
            total = added if total is None else total + added
    out_ref[...] = total.astype(jnp.bfloat16)


def on_device(q_nope, q_rope, c_kv, k_rope, positions, w_uk, w_uv, w_out):
    toks, lat = c_kv.shape
    heads, tile_rows, _ = w_uk.shape
    ranks = lax.axis_size("ctx")
    planes = lax.axis_size("tp")
    chips = ranks // CORES
    assert heads == chips
    nope = tile_rows * ranks
    rope = k_rope.shape[1]
    v_rows, v_dim = w_uv.shape[1:]
    scale = (nope + rope) ** (-0.5)
    same_core = [[z * CORES + k for z in range(chips)] for k in range(CORES)]
    one_chip = [[z * CORES + k for k in range(CORES)] for z in range(chips)]

    plane = lax.axis_index("tp")
    share = toks // planes

    def cut_share(a):
        return lax.dynamic_slice_in_dim(a, plane * share, share, 0)

    own_pos = cut_share(positions)
    k_rot = rotate(cut_share(k_rope), *cos_sin(own_pos, rope // 2)).astype(jnp.bfloat16)
    digits = jnp.stack([own_pos // DIGIT, own_pos % DIGIT], axis=1).astype(jnp.bfloat16)
    zeros = jnp.zeros((share, LANES - rope - 2), jnp.bfloat16)
    own_keys = jnp.concatenate([cut_share(c_kv), k_rot, digits, zeros], axis=1)
    own_keys = jnp.broadcast_to(own_keys, (chips, *own_keys.shape))
    own_keys = lax.all_to_all(
        own_keys, "ctx", split_axis=0, concat_axis=0, tiled=True, axis_index_groups=same_core
    )
    own_keys = lax.all_gather(own_keys.reshape(chips * share, -1), "tp", axis=0, tiled=True)
    swap = [(r, r // CORES * CORES + (r + 1) % CORES) for r in range(ranks)]
    other_keys = lax.ppermute(own_keys, "ctx", swap)

    cosine, sine = cos_sin(positions, rope // 2)
    q_parts = q_nope.reshape(toks, heads, nope).transpose(1, 0, 2)
    q_rot = rotate(q_rope.reshape(toks, heads, rope), cosine[:, None], sine[:, None])
    q_rot = q_rot.astype(jnp.bfloat16).transpose(1, 0, 2)
    q_rot = jnp.concatenate([q_rot[:, : toks // 2], q_rot[:, toks // 2 :]], axis=2)
    k_rows = tile_rows * lat // LANES
    sent = jnp.concatenate([q_parts, q_rot, w_uk.reshape(heads, k_rows, LANES), w_uv], axis=1)
    came = lax.all_to_all(
        sent, "ctx", split_axis=0, concat_axis=0, tiled=True, axis_index_groups=same_core
    )
    cut = toks + toks // 2
    q_parts = came[:, :toks].reshape(chips * toks, nope)
    q_rot = came[:, toks:cut]
    q_rot = jnp.concatenate([q_rot[:, :, :rope], q_rot[:, :, rope:]], axis=1).reshape(-1, rope)
    both = jnp.broadcast_to(came[None, :, cut:], (CORES, chips, k_rows + v_rows, LANES))
    both = lax.all_to_all(
        both, "ctx", split_axis=0, concat_axis=0, tiled=True, axis_index_groups=one_chip
    )
    both = both.transpose(1, 0, 2, 3)
    up_key = both[:, :, :k_rows].reshape(nope, lat)
    up_value = both[:, :, k_rows:].reshape(lat, v_dim)
    q_lat = jnp.dot(q_parts, up_key, preferred_element_type=jnp.float32).astype(jnp.bfloat16)
    queries = jnp.concatenate(
        [q_lat, q_rot, jnp.zeros((chips * toks, LANES - rope), jnp.bfloat16)], axis=1
    )

    own_w = w_out.T
    right = [(i, (i + 1) % planes) for i in range(planes)]
    left = [(i, (i - 1) % planes) for i in range(planes)]
    all_w = jnp.zeros((planes, *own_w.shape), jnp.bfloat16)

    def placed(stack, block, shift):
        return lax.dynamic_update_slice(stack, block[None], ((plane + shift) % planes, 0, 0))

    lower = lax.ppermute(own_w, "tp", right)
    all_w = placed(placed(all_w, own_w, 0), lower, planes - 1)
    upper = own_w

    vmem = pl.BlockSpec(memory_space=pltpu.VMEM)
    hbm = pl.BlockSpec(memory_space=pl.ANY)
    block = min(256, chips * toks)
    head_out = pl.pallas_call(
        functools.partial(attend, chips, planes, toks, lat, scale, block),
        out_shape=jax.ShapeDtypeStruct((chips * toks, v_dim), jnp.bfloat16),
        in_specs=[vmem, vmem, vmem, vmem],
        out_specs=vmem,
        scratch_shapes=[pltpu.VMEM((chips, planes, share, LANES), jnp.float32)],
    )(queries, up_value, own_keys, other_keys)

    by_plane = lax.all_to_all(
        head_out.reshape(planes, -1, v_dim), "tp", split_axis=0, concat_axis=0, tiled=True
    )
    gathered = lax.all_gather(by_plane.reshape(-1, v_dim), "ctx", axis=0)
    gathered = gathered.reshape(chips, CORES, planes, -1, v_dim)
    for s in range(1, planes // 2):
        lower = lax.ppermute(lower, "tp", right)
        upper = lax.ppermute(upper, "tp", left)
        all_w = placed(placed(all_w, lower, planes - 1 - s), upper, s)

    out_toks = gathered.shape[3] * CORES
    columns = w_out.shape[1]
    steps = 8
    out = pl.pallas_call(
        functools.partial(project, chips, planes, toks, steps),
        out_shape=jax.ShapeDtypeStruct((columns, out_toks), jnp.bfloat16),
        in_specs=[hbm, hbm],
        out_specs=vmem,
        scratch_shapes=[
            pltpu.VMEM((chips, planes, out_toks, v_dim), jnp.bfloat16),
            pltpu.VMEM((steps, planes, columns, chips // steps * v_dim), jnp.bfloat16),
            pltpu.SemaphoreType.DMA((steps, 1 + out_toks // toks)),
        ],
    )(gathered, all_w)
    return out.T


def solution(mesh):
    in_specs = (
        P(("groups", "ctx"), "tp"),
        P(("groups", "ctx"), "tp"),
        P(("groups", "ctx"), None),
        P(("groups", "ctx"), None),
        P(("groups", "ctx")),
        P("tp", "ctx", None),
        P("tp", "ctx", None),
        P("tp", "ctx"),
    )
    out_specs = P(("groups", "tp"), "ctx")

    return jax.shard_map(on_device, mesh=mesh, in_specs=in_specs, out_specs=out_specs, check_vma=False)
```

```python
import functools

import jax
import jax.numpy as jnp
from jax import lax
from jax.experimental import pallas as pl
from jax.experimental.pallas import tpu as pltpu
from jax.sharding import PartitionSpec as P


LANES = 128
DIGIT = 32
CORES = 2


def cos_sin(position, half_dim):
    freqs = 10000.0 ** (-jnp.arange(half_dim, dtype=jnp.float32) / half_dim)
    angles = position.astype(jnp.float32)[..., None] * freqs
    return jnp.cos(angles), jnp.sin(angles)


def rotate(values, cosine, sine):
    half_dim = values.shape[-1] // 2
    first_half = values[..., :half_dim].astype(jnp.float32)
    second_half = values[..., half_dim:].astype(jnp.float32)
    return jnp.concatenate(
        [first_half * cosine - second_half * sine, second_half * cosine + first_half * sine],
        axis=-1,
    )


def attend(chips, planes, toks, lat, scale, block, q_ref, wv_ref, own_ref, other_ref, out_ref, pos_buf):
    share = toks // planes
    half = LANES // 2
    lane = lax.broadcasted_iota(jnp.int32, (LANES, LANES), 1)
    pick = jnp.where(lane == half, float(DIGIT), jnp.where(lane == half + 1, 1.0, 0.0))
    pick = pick.astype(jnp.bfloat16)
    nt = (((1,), (1,)), ((), ()))
    all_keys = jnp.concatenate([own_ref[...], other_ref[...]], axis=0)
    key_pos = lax.dot_general(pick[0:8], all_keys[:, lat:], nt, preferred_element_type=jnp.float32)[0:1]
    own_pos = lax.dot_general(own_ref[:, lat:], pick, nt, preferred_element_type=jnp.float32)
    own_pos = own_pos.reshape(planes, chips, share, LANES)
    for x in range(planes):
        pos_buf[:, x] = own_pos[x]
    q_pos = pos_buf[...].reshape(chips * toks, LANES)[:, 0:1]
    factor = scale * 1.4426950408889634
    blocks = [slice(at, at + block) for at in range(0, chips * toks, block)]

    def score(rows):
        return lax.dot_general(q_ref[rows, :], all_keys, nt, preferred_element_type=jnp.float32)

    following = score(blocks[0])
    for b, rows in enumerate(blocks):
        scores = jnp.where(key_pos <= q_pos[rows], following, -1e30)
        if b + 1 < len(blocks):
            following = score(blocks[b + 1])
        top = jnp.max(scores, axis=1, keepdims=True)
        weights = jnp.exp2((scores - top) * factor)
        total = jnp.sum(weights, axis=1, keepdims=True)
        mixed = jnp.dot(
            weights.astype(jnp.bfloat16), all_keys[:, :lat], preferred_element_type=jnp.float32
        )
        o_lat = (mixed * (1.0 / total)).astype(jnp.bfloat16)
        out_ref[rows, :] = jnp.dot(
            o_lat, wv_ref[...], preferred_element_type=jnp.float32
        ).astype(jnp.bfloat16)


def project(chips, planes, toks, steps, gathered, weights, out_ref, heads_buf, w_buf, sems):
    each = chips // steps
    pairs = heads_buf.shape[2] // (CORES * toks)
    v_dim = heads_buf.shape[3]
    copies = []
    for s in range(steps):
        zs = slice(s * each, (s + 1) * each)
        group = [
            pltpu.make_async_copy(
                weights.at[:, :, s * each * v_dim : (s + 1) * each * v_dim], w_buf.at[s], sems.at[s, 0]
            )
        ]
        for pair in range(pairs):
            for k in range(CORES):
                at = (pair * CORES + k) * toks
                group.append(
                    pltpu.make_async_copy(
                        gathered.at[zs, k, :, pair * toks : (pair + 1) * toks, :],
                        heads_buf.at[zs, :, at : at + toks, :],
                        sems.at[s, 1 + pair * CORES + k],
                    )
                )
        copies.append(group)
    for group in copies:
        for c in group:
            c.start()
    total = None
    for s in range(steps):
        for c in copies[s]:
            c.wait()
        for i in range(each):
            z = s * each + i
            rows = jnp.concatenate([heads_buf[z, x] for x in range(planes)], axis=1)
            w = jnp.concatenate(
                [w_buf[s, x, :, i * v_dim : (i + 1) * v_dim] for x in range(planes)], axis=1
            )
            added = lax.dot_general(
                w, rows, (((1,), (1,)), ((), ())), preferred_element_type=jnp.float32
            )
            total = added if total is None else total + added
    out_ref[...] = total.astype(jnp.bfloat16)


def on_device(q_nope, q_rope, c_kv, k_rope, positions, w_uk, w_uv, w_out):
    toks, lat = c_kv.shape
    heads, tile_rows, _ = w_uk.shape
    ranks = lax.axis_size("ctx")
    planes = lax.axis_size("tp")
    chips = ranks // CORES
    assert heads == chips
    nope = tile_rows * ranks
    rope = k_rope.shape[1]
    v_rows, v_dim = w_uv.shape[1:]
    scale = (nope + rope) ** (-0.5)
    same_core = [[z * CORES + k for z in range(chips)] for k in range(CORES)]
    one_chip = [[z * CORES + k for k in range(CORES)] for z in range(chips)]

    plane = lax.axis_index("tp")
    share = toks // planes

    def cut_share(a):
        return lax.dynamic_slice_in_dim(a, plane * share, share, 0)

    own_pos = cut_share(positions)
    k_rot = rotate(cut_share(k_rope), *cos_sin(own_pos, rope // 2)).astype(jnp.bfloat16)
    digits = jnp.stack([own_pos // DIGIT, own_pos % DIGIT], axis=1).astype(jnp.bfloat16)
    zeros = jnp.zeros((share, LANES - rope - 2), jnp.bfloat16)
    own_keys = jnp.concatenate([cut_share(c_kv), k_rot, digits, zeros], axis=1)
    own_keys = jnp.broadcast_to(own_keys, (chips, *own_keys.shape))
    own_keys = lax.all_to_all(
        own_keys, "ctx", split_axis=0, concat_axis=0, tiled=True, axis_index_groups=same_core
    )
    own_keys = lax.all_gather(own_keys.reshape(chips * share, -1), "tp", axis=0, tiled=True)
    swap = [(r, r // CORES * CORES + (r + 1) % CORES) for r in range(ranks)]
    other_keys = lax.ppermute(own_keys, "ctx", swap)

    cosine, sine = cos_sin(positions, rope // 2)
    q_parts = q_nope.reshape(toks, heads, nope).transpose(1, 0, 2)
    q_rot = rotate(q_rope.reshape(toks, heads, rope), cosine[:, None], sine[:, None])
    q_rot = q_rot.astype(jnp.bfloat16).transpose(1, 0, 2)
    q_rot = jnp.concatenate([q_rot[:, : toks // 2], q_rot[:, toks // 2 :]], axis=2)
    k_rows = tile_rows * lat // LANES
    sent = jnp.concatenate([q_parts, q_rot, w_uk.reshape(heads, k_rows, LANES), w_uv], axis=1)
    came = lax.all_to_all(
        sent, "ctx", split_axis=0, concat_axis=0, tiled=True, axis_index_groups=same_core
    )
    cut = toks + toks // 2
    q_parts = came[:, :toks].reshape(chips * toks, nope)
    q_rot = came[:, toks:cut]
    q_rot = jnp.concatenate([q_rot[:, :, :rope], q_rot[:, :, rope:]], axis=1).reshape(-1, rope)
    both = jnp.broadcast_to(came[None, :, cut:], (CORES, chips, k_rows + v_rows, LANES))
    both = lax.all_to_all(
        both, "ctx", split_axis=0, concat_axis=0, tiled=True, axis_index_groups=one_chip
    )
    both = both.transpose(1, 0, 2, 3)
    up_key = both[:, :, :k_rows].reshape(nope, lat)
    up_value = both[:, :, k_rows:].reshape(lat, v_dim)
    q_lat = jnp.dot(q_parts, up_key, preferred_element_type=jnp.float32).astype(jnp.bfloat16)
    queries = jnp.concatenate(
        [q_lat, q_rot, jnp.zeros((chips * toks, LANES - rope), jnp.bfloat16)], axis=1
    )

    own_w = w_out.T
    right = [(i, (i + 1) % planes) for i in range(planes)]
    left = [(i, (i - 1) % planes) for i in range(planes)]
    all_w = jnp.zeros((planes, *own_w.shape), jnp.bfloat16)

    def placed(stack, block, shift):
        return lax.dynamic_update_slice(stack, block[None], ((plane + shift) % planes, 0, 0))

    lower = lax.ppermute(own_w, "tp", right)
    all_w = placed(placed(all_w, own_w, 0), lower, planes - 1)
    upper = own_w

    vmem = pl.BlockSpec(memory_space=pltpu.VMEM)
    hbm = pl.BlockSpec(memory_space=pl.ANY)
    block = min(256, chips * toks)
    head_out = pl.pallas_call(
        functools.partial(attend, chips, planes, toks, lat, scale, block),
        out_shape=jax.ShapeDtypeStruct((chips * toks, v_dim), jnp.bfloat16),
        in_specs=[vmem, vmem, vmem, vmem],
        out_specs=vmem,
        scratch_shapes=[pltpu.VMEM((chips, planes, share, LANES), jnp.float32)],
        compiler_params=pltpu.CompilerParams(vmem_limit_bytes=20 * 2**20),
    )(queries, up_value, own_keys, other_keys)

    by_plane = lax.all_to_all(
        head_out.reshape(planes, -1, v_dim), "tp", split_axis=0, concat_axis=0, tiled=True
    )
    gathered = lax.all_gather(by_plane.reshape(-1, v_dim), "ctx", axis=0)
    gathered = gathered.reshape(chips, CORES, planes, -1, v_dim)
    for s in range(1, planes // 2):
        lower = lax.ppermute(lower, "tp", right)
        upper = lax.ppermute(upper, "tp", left)
        all_w = placed(placed(all_w, lower, planes - 1 - s), upper, s)

    out_toks = gathered.shape[3] * CORES
    columns = w_out.shape[1]
    steps = 8
    out = pl.pallas_call(
        functools.partial(project, chips, planes, toks, steps),
        out_shape=jax.ShapeDtypeStruct((columns, out_toks), jnp.bfloat16),
        in_specs=[hbm, hbm],
        out_specs=vmem,
        scratch_shapes=[
            pltpu.VMEM((chips, planes, out_toks, v_dim), jnp.bfloat16),
            pltpu.VMEM((steps, planes, columns, chips // steps * v_dim), jnp.bfloat16),
            pltpu.SemaphoreType.DMA((steps, 1 + out_toks // toks)),
        ],
    )(gathered, all_w)
    return out.T


def solution(mesh):
    in_specs = (
        P(("groups", "ctx"), "tp"),
        P(("groups", "ctx"), "tp"),
        P(("groups", "ctx"), None),
        P(("groups", "ctx"), None),
        P(("groups", "ctx")),
        P("tp", "ctx", None),
        P("tp", "ctx", None),
        P("tp", "ctx"),
    )
    out_specs = P(("groups", "tp"), "ctx")

    return jax.shard_map(on_device, mesh=mesh, in_specs=in_specs, out_specs=out_specs, check_vma=False)
```

```python
import functools

import jax
import jax.numpy as jnp
from jax import lax
from jax.experimental import pallas as pl
from jax.experimental.pallas import tpu as pltpu
from jax.sharding import PartitionSpec as P


LANES = 128
DIGIT = 32
CORES = 2


def cos_sin(position, half_dim):
    freqs = 10000.0 ** (-jnp.arange(half_dim, dtype=jnp.float32) / half_dim)
    angles = position.astype(jnp.float32)[..., None] * freqs
    return jnp.cos(angles), jnp.sin(angles)


def rotate(values, cosine, sine):
    half_dim = values.shape[-1] // 2
    first_half = values[..., :half_dim].astype(jnp.float32)
    second_half = values[..., half_dim:].astype(jnp.float32)
    return jnp.concatenate(
        [first_half * cosine - second_half * sine, second_half * cosine + first_half * sine],
        axis=-1,
    )


def attend(chips, planes, toks, lat, scale, block, q_ref, wv_ref, own_ref, other_ref, out_ref, pos_buf):
    share = toks // planes
    half = LANES // 2
    lane = lax.broadcasted_iota(jnp.int32, (LANES, LANES), 1)
    pick = jnp.where(lane == half, float(DIGIT), jnp.where(lane == half + 1, 1.0, 0.0))
    pick = pick.astype(jnp.bfloat16)
    nt = (((1,), (1,)), ((), ()))
    all_keys = jnp.concatenate([own_ref[...], other_ref[...]], axis=0)
    key_pos = lax.dot_general(pick[0:8], all_keys[:, lat:], nt, preferred_element_type=jnp.float32)[0:1]
    own_pos = lax.dot_general(own_ref[:, lat:], pick, nt, preferred_element_type=jnp.float32)
    own_pos = own_pos.reshape(planes, chips, share, LANES)
    for x in range(planes):
        pos_buf[:, x] = own_pos[x]
    q_pos = pos_buf[...].reshape(chips * toks, LANES)[:, 0:1]
    factor = scale * 1.4426950408889634
    blocks = [slice(at, at + block) for at in range(0, chips * toks, block)]

    def score(rows):
        return lax.dot_general(q_ref[rows, :], all_keys, nt, preferred_element_type=jnp.float32)

    following = score(blocks[0])
    for b, rows in enumerate(blocks):
        scores = jnp.where(key_pos <= q_pos[rows], following, -1e30)
        if b + 1 < len(blocks):
            following = score(blocks[b + 1])
        top = jnp.max(scores, axis=1, keepdims=True)
        weights = jnp.exp2((scores - top) * factor)
        total = jnp.sum(weights, axis=1, keepdims=True)
        mixed = jnp.dot(
            weights.astype(jnp.bfloat16), all_keys[:, :lat], preferred_element_type=jnp.float32
        )
        o_lat = (mixed * (1.0 / total)).astype(jnp.bfloat16)
        out_ref[rows, :] = jnp.dot(
            o_lat, wv_ref[...], preferred_element_type=jnp.float32
        ).astype(jnp.bfloat16)


def project(chips, planes, toks, steps, gathered, weights, out_ref, heads_buf, w_buf, sems):
    each = chips // steps
    pairs = heads_buf.shape[2] // (CORES * toks)
    v_dim = heads_buf.shape[3]
    copies = []
    for s in range(steps):
        zs = slice(s * each, (s + 1) * each)
        group = [
            pltpu.make_async_copy(
                weights.at[:, :, s * each * v_dim : (s + 1) * each * v_dim], w_buf.at[s], sems.at[s, 0]
            )
        ]
        for pair in range(pairs):
            for k in range(CORES):
                at = (pair * CORES + k) * toks
                group.append(
                    pltpu.make_async_copy(
                        gathered.at[zs, k, :, pair * toks : (pair + 1) * toks, :],
                        heads_buf.at[zs, :, at : at + toks, :],
                        sems.at[s, 1 + pair * CORES + k],
                    )
                )
        copies.append(group)
    for group in copies:
        for c in group:
            c.start()
    total = None
    for s in range(steps):
        for c in copies[s]:
            c.wait()
        for i in range(each):
            z = s * each + i
            rows = jnp.concatenate([heads_buf[z, x] for x in range(planes)], axis=1)
            w = jnp.concatenate(
                [w_buf[s, x, :, i * v_dim : (i + 1) * v_dim] for x in range(planes)], axis=1
            )
            added = lax.dot_general(
                w, rows, (((1,), (1,)), ((), ())), preferred_element_type=jnp.float32
            )
            total = added if total is None else total + added
    out_ref[...] = total.astype(jnp.bfloat16)


def on_device(q_nope, q_rope, c_kv, k_rope, positions, w_uk, w_uv, w_out):
    toks, lat = c_kv.shape
    heads, tile_rows, _ = w_uk.shape
    ranks = lax.axis_size("ctx")
    planes = lax.axis_size("tp")
    chips = ranks // CORES
    assert heads == chips
    nope = tile_rows * ranks
    rope = k_rope.shape[1]
    _, v_dim = w_uv.shape[1:]
    scale = (nope + rope) ** (-0.5)
    same_core = [[z * CORES + k for z in range(chips)] for k in range(CORES)]

    plane = lax.axis_index("tp")
    share = toks // planes

    def cut_share(a):
        return lax.dynamic_slice_in_dim(a, plane * share, share, 0)

    own_pos = cut_share(positions)
    k_rot = rotate(cut_share(k_rope), *cos_sin(own_pos, rope // 2)).astype(jnp.bfloat16)
    digits = jnp.stack([own_pos // DIGIT, own_pos % DIGIT], axis=1).astype(jnp.bfloat16)
    zeros = jnp.zeros((share, LANES - rope - 2), jnp.bfloat16)
    own_keys = jnp.concatenate([cut_share(c_kv), k_rot, digits, zeros], axis=1)
    own_keys = jnp.broadcast_to(own_keys, (chips, *own_keys.shape))
    own_keys = lax.all_to_all(
        own_keys, "ctx", split_axis=0, concat_axis=0, tiled=True, axis_index_groups=same_core
    )
    own_keys = lax.all_gather(own_keys.reshape(chips * share, -1), "tp", axis=0, tiled=True)
    swap = [(r, r // CORES * CORES + (r + 1) % CORES) for r in range(ranks)]
    other_keys = lax.ppermute(own_keys, "ctx", swap)

    cosine, sine = cos_sin(positions, rope // 2)
    q_parts = q_nope.reshape(toks, heads, nope).transpose(1, 0, 2)
    q_rot = rotate(q_rope.reshape(toks, heads, rope), cosine[:, None], sine[:, None])
    q_rot = q_rot.astype(jnp.bfloat16).transpose(1, 0, 2)
    q_rot = jnp.concatenate([q_rot[:, : toks // 2], q_rot[:, toks // 2 :]], axis=2)
    k_rows = tile_rows * lat // LANES
    sent = jnp.concatenate([q_parts, q_rot, w_uk.reshape(heads, k_rows, LANES), w_uv], axis=1)
    came = lax.all_to_all(
        sent, "ctx", split_axis=0, concat_axis=0, tiled=True, axis_index_groups=same_core
    )
    cut = toks + toks // 2
    q_parts = came[:, :toks].reshape(chips * toks, nope)
    q_rot = came[:, toks:cut]
    q_rot = jnp.concatenate([q_rot[:, :, :rope], q_rot[:, :, rope:]], axis=1).reshape(-1, rope)
    own_up = came[:, cut:]
    other_up = lax.ppermute(own_up, "ctx", swap)
    is_first = lax.axis_index("ctx") % CORES == 0
    both = jnp.stack(
        [jnp.where(is_first, own_up, other_up), jnp.where(is_first, other_up, own_up)], axis=1
    )
    up_key = both[:, :, :k_rows].reshape(nope, lat)
    up_value = both[:, :, k_rows:].reshape(lat, v_dim)
    q_lat = jnp.dot(q_parts, up_key, preferred_element_type=jnp.float32).astype(jnp.bfloat16)
    queries = jnp.concatenate(
        [q_lat, q_rot, jnp.zeros((chips * toks, LANES - rope), jnp.bfloat16)], axis=1
    )

    own_w = w_out.T
    right = [(i, (i + 1) % planes) for i in range(planes)]
    left = [(i, (i - 1) % planes) for i in range(planes)]
    all_w = jnp.zeros((planes, *own_w.shape), jnp.bfloat16)

    part_columns = own_w.shape[0] // 2
    halves = [own_w[:part_columns], own_w[part_columns:]]

    def placed(stack, block, shift, half):
        at = ((plane + shift) % planes, half * part_columns, 0)
        return lax.dynamic_update_slice(stack, block[None], at)

    vmem = pl.BlockSpec(memory_space=pltpu.VMEM)
    hbm = pl.BlockSpec(memory_space=pl.ANY)
    block = min(256, chips * toks)
    head_out = pl.pallas_call(
        functools.partial(attend, chips, planes, toks, lat, scale, block),
        out_shape=jax.ShapeDtypeStruct((chips * toks, v_dim), jnp.bfloat16),
        in_specs=[vmem, vmem, vmem, vmem],
        out_specs=vmem,
        scratch_shapes=[pltpu.VMEM((chips, planes, share, LANES), jnp.float32)],
        compiler_params=pltpu.CompilerParams(vmem_limit_bytes=20 * 2**20),
    )(queries, up_value, own_keys, other_keys)

    by_plane = lax.all_to_all(
        head_out.reshape(planes, -1, v_dim), "tp", split_axis=0, concat_axis=0, tiled=True
    )
    gathered = lax.all_gather(by_plane.reshape(-1, v_dim), "ctx", axis=0)
    gathered = gathered.reshape(chips, CORES, planes, -1, v_dim)
    for half in range(2):
        all_w = placed(all_w, halves[half], 0, half)
    upward, downward = list(halves), list(halves)
    for s in range(1, planes // 2 + 1):
        for i in range(2):
            for half, moving, to, shift in ((i, upward, right, -s), (1 - i, downward, left, s)):
                if i == 0 or 2 * s < planes:
                    moving[half] = lax.ppermute(moving[half], "tp", to)
                    all_w = placed(all_w, moving[half], planes + shift, half)

    out_toks = gathered.shape[3] * CORES
    columns = w_out.shape[1]
    steps = 8
    out = pl.pallas_call(
        functools.partial(project, chips, planes, toks, steps),
        out_shape=jax.ShapeDtypeStruct((columns, out_toks), jnp.bfloat16),
        in_specs=[hbm, hbm],
        out_specs=vmem,
        scratch_shapes=[
            pltpu.VMEM((chips, planes, out_toks, v_dim), jnp.bfloat16),
            pltpu.VMEM((steps, planes, columns, chips // steps * v_dim), jnp.bfloat16),
            pltpu.SemaphoreType.DMA((steps, 1 + out_toks // toks)),
        ],
    )(gathered, all_w)
    return out.T


def solution(mesh):
    in_specs = (
        P(("groups", "ctx"), "tp"),
        P(("groups", "ctx"), "tp"),
        P(("groups", "ctx"), None),
        P(("groups", "ctx"), None),
        P(("groups", "ctx")),
        P("tp", "ctx", None),
        P("tp", "ctx", None),
        P("tp", "ctx"),
    )
    out_specs = P(("groups", "tp"), "ctx")

    return jax.shard_map(on_device, mesh=mesh, in_specs=in_specs, out_specs=out_specs, check_vma=False)
```

```python
import functools

import jax
import jax.numpy as jnp
import numpy as np
from jax import lax
from jax.experimental import pallas as pl
from jax.experimental.pallas import tpu as pltpu
from jax.sharding import PartitionSpec as P


LANES = 128
DIGIT = 32
CORES = 2


def frequencies(half_dim):
    return np.power(10000.0, -np.arange(half_dim) / half_dim).astype(np.float32)


def rotate(values, cosine, sine):
    half_dim = values.shape[-1] // 2
    first_half = values[..., :half_dim].astype(jnp.float32)
    second_half = values[..., half_dim:].astype(jnp.float32)
    return jnp.concatenate(
        [first_half * cosine - second_half * sine, second_half * cosine + first_half * sine],
        axis=-1,
    )


def prepare(chips, share, plane_ref, positions_ref, freqs_ref, c_kv_ref, k_rope_ref, out_ref):
    at = pl.multiple_of(plane_ref[0] * share, share)
    position = positions_ref[at] + lax.broadcasted_iota(jnp.int32, (share, 1), 0)
    angles = position.astype(jnp.float32) * freqs_ref[...]
    rotated = rotate(k_rope_ref[pl.ds(at, share), :], jnp.cos(angles), jnp.sin(angles))
    lane = lax.broadcasted_iota(jnp.int32, (share, LANES - rotated.shape[1]), 1)
    digits = jnp.where(lane == 0, position // DIGIT, jnp.where(lane == 1, position % DIGIT, 0))
    row = jnp.concatenate([rotated, digits.astype(jnp.float32)], axis=1).astype(jnp.bfloat16)
    row = jnp.concatenate([c_kv_ref[pl.ds(at, share), :], row], axis=1)
    for z in range(chips):
        out_ref[z] = row


def attend(chips, planes, toks, lat, scale, block, q_ref, wv_ref, own_ref, other_ref, out_ref, pos_buf):
    share = toks // planes
    half = LANES // 2
    lane = lax.broadcasted_iota(jnp.int32, (LANES, LANES), 1)
    pick = jnp.where(lane == half, float(DIGIT), jnp.where(lane == half + 1, 1.0, 0.0))
    pick = pick.astype(jnp.bfloat16)
    nt = (((1,), (1,)), ((), ()))
    all_keys = jnp.concatenate([own_ref[...], other_ref[...]], axis=0)
    key_pos = lax.dot_general(pick[0:8], all_keys[:, lat:], nt, preferred_element_type=jnp.float32)[0:1]
    own_pos = lax.dot_general(own_ref[:, lat:], pick, nt, preferred_element_type=jnp.float32)
    own_pos = own_pos.reshape(planes, chips, share, LANES)
    for x in range(planes):
        pos_buf[:, x] = own_pos[x]
    q_pos = pos_buf[...].reshape(chips * toks, LANES)[:, 0:1]
    factor = scale * 1.4426950408889634
    blocks = [slice(at, at + block) for at in range(0, chips * toks, block)]

    def score(rows):
        return lax.dot_general(q_ref[rows, :], all_keys, nt, preferred_element_type=jnp.float32)

    following = score(blocks[0])
    for b, rows in enumerate(blocks):
        scores = jnp.where(key_pos <= q_pos[rows], following, -1e30)
        if b + 1 < len(blocks):
            following = score(blocks[b + 1])
        top = jnp.max(scores, axis=1, keepdims=True)
        weights = jnp.exp2((scores - top) * factor)
        total = jnp.sum(weights, axis=1, keepdims=True)
        mixed = jnp.dot(
            weights.astype(jnp.bfloat16), all_keys[:, :lat], preferred_element_type=jnp.float32
        )
        o_lat = (mixed * (1.0 / total)).astype(jnp.bfloat16)
        out_ref[rows, :] = jnp.dot(
            o_lat, wv_ref[...], preferred_element_type=jnp.float32
        ).astype(jnp.bfloat16)


def project(chips, planes, toks, steps, gathered, weights, out_ref, heads_buf, w_buf, sems):
    each = chips // steps
    pairs = heads_buf.shape[2] // (CORES * toks)
    v_dim = heads_buf.shape[3]
    copies = []
    for s in range(steps):
        zs = slice(s * each, (s + 1) * each)
        group = [
            pltpu.make_async_copy(
                weights.at[:, :, s * each * v_dim : (s + 1) * each * v_dim], w_buf.at[s], sems.at[s, 0]
            )
        ]
        for pair in range(pairs):
            for k in range(CORES):
                at = (pair * CORES + k) * toks
                group.append(
                    pltpu.make_async_copy(
                        gathered.at[zs, k, :, pair * toks : (pair + 1) * toks, :],
                        heads_buf.at[zs, :, at : at + toks, :],
                        sems.at[s, 1 + pair * CORES + k],
                    )
                )
        copies.append(group)
    for group in copies:
        for c in group:
            c.start()
    total = None
    for s in range(steps):
        for c in copies[s]:
            c.wait()
        for i in range(each):
            z = s * each + i
            rows = jnp.concatenate([heads_buf[z, x] for x in range(planes)], axis=1)
            w = jnp.concatenate(
                [w_buf[s, x, :, i * v_dim : (i + 1) * v_dim] for x in range(planes)], axis=1
            )
            added = lax.dot_general(
                w, rows, (((1,), (1,)), ((), ())), preferred_element_type=jnp.float32
            )
            total = added if total is None else total + added
    out_ref[...] = total.astype(jnp.bfloat16)


def on_device(q_nope, q_rope, c_kv, k_rope, positions, w_uk, w_uv, w_out):
    toks, lat = c_kv.shape
    heads, tile_rows, _ = w_uk.shape
    ranks = lax.axis_size("ctx")
    planes = lax.axis_size("tp")
    chips = ranks // CORES
    assert heads == chips
    nope = tile_rows * ranks
    rope = k_rope.shape[1]
    v_rows, v_dim = w_uv.shape[1:]
    scale = (nope + rope) ** (-0.5)
    same_core = [[z * CORES + k for z in range(chips)] for k in range(CORES)]
    one_chip = [[z * CORES + k for k in range(CORES)] for z in range(chips)]

    plane = lax.axis_index("tp")
    share = toks // planes

    assert DIGIT % share == 0
    vmem = pl.BlockSpec(memory_space=pltpu.VMEM)
    smem = pl.BlockSpec(memory_space=pltpu.SMEM)
    freqs = jnp.asarray(frequencies(rope // 2))[None]
    own_keys = pl.pallas_call(
        functools.partial(prepare, chips, share),
        out_shape=jax.ShapeDtypeStruct((chips, share, lat + LANES), jnp.bfloat16),
        in_specs=[smem, smem, vmem, vmem, vmem],
        out_specs=vmem,
    )(plane.astype(jnp.int32).reshape(1), positions, freqs, c_kv, k_rope)
    own_keys = lax.all_to_all(
        own_keys, "ctx", split_axis=0, concat_axis=0, tiled=True, axis_index_groups=same_core
    )
    own_keys = lax.all_gather(own_keys.reshape(chips * share, -1), "tp", axis=0, tiled=True)
    swap = [(r, r // CORES * CORES + (r + 1) % CORES) for r in range(ranks)]
    other_keys = lax.ppermute(own_keys, "ctx", swap)

    angles = positions.astype(jnp.float32)[:, None] * freqs
    cosine, sine = jnp.cos(angles), jnp.sin(angles)
    q_parts = q_nope.reshape(toks, heads, nope).transpose(1, 0, 2)
    q_rot = rotate(q_rope.reshape(toks, heads, rope), cosine[:, None], sine[:, None])
    q_rot = q_rot.astype(jnp.bfloat16).transpose(1, 0, 2)
    q_rot = jnp.concatenate([q_rot[:, : toks // 2], q_rot[:, toks // 2 :]], axis=2)
    k_rows = tile_rows * lat // LANES
    sent = jnp.concatenate([q_parts, q_rot, w_uk.reshape(heads, k_rows, LANES), w_uv], axis=1)
    came = lax.all_to_all(
        sent, "ctx", split_axis=0, concat_axis=0, tiled=True, axis_index_groups=same_core
    )
    cut = toks + toks // 2
    q_parts = came[:, :toks].reshape(chips * toks, nope)
    q_rot = came[:, toks:cut]
    q_rot = jnp.concatenate([q_rot[:, :, :rope], q_rot[:, :, rope:]], axis=1).reshape(-1, rope)
    both = jnp.broadcast_to(came[None, :, cut:], (CORES, chips, k_rows + v_rows, LANES))
    both = lax.all_to_all(
        both, "ctx", split_axis=0, concat_axis=0, tiled=True, axis_index_groups=one_chip
    )
    both = both.transpose(1, 0, 2, 3)
    up_key = both[:, :, :k_rows].reshape(nope, lat)
    up_value = both[:, :, k_rows:].reshape(lat, v_dim)
    q_lat = jnp.dot(q_parts, up_key, preferred_element_type=jnp.float32).astype(jnp.bfloat16)
    queries = jnp.concatenate(
        [q_lat, q_rot, jnp.zeros((chips * toks, LANES - rope), jnp.bfloat16)], axis=1
    )

    own_w = w_out.T
    right = [(i, (i + 1) % planes) for i in range(planes)]
    left = [(i, (i - 1) % planes) for i in range(planes)]
    all_w = jnp.zeros((planes, *own_w.shape), jnp.bfloat16)

    def placed(stack, block, shift):
        return lax.dynamic_update_slice(stack, block[None], ((plane + shift) % planes, 0, 0))

    lower = lax.ppermute(own_w, "tp", right)
    all_w = placed(placed(all_w, own_w, 0), lower, planes - 1)
    upper = own_w

    hbm = pl.BlockSpec(memory_space=pl.ANY)
    block = min(256, chips * toks)
    head_out = pl.pallas_call(
        functools.partial(attend, chips, planes, toks, lat, scale, block),
        out_shape=jax.ShapeDtypeStruct((chips * toks, v_dim), jnp.bfloat16),
        in_specs=[vmem, vmem, vmem, vmem],
        out_specs=vmem,
        scratch_shapes=[pltpu.VMEM((chips, planes, share, LANES), jnp.float32)],
        compiler_params=pltpu.CompilerParams(vmem_limit_bytes=20 * 2**20),
    )(queries, up_value, own_keys, other_keys)

    by_plane = lax.all_to_all(
        head_out.reshape(planes, -1, v_dim), "tp", split_axis=0, concat_axis=0, tiled=True
    )
    gathered = lax.all_gather(by_plane.reshape(-1, v_dim), "ctx", axis=0)
    gathered = gathered.reshape(chips, CORES, planes, -1, v_dim)
    for s in range(1, planes // 2):
        lower = lax.ppermute(lower, "tp", right)
        upper = lax.ppermute(upper, "tp", left)
        all_w = placed(placed(all_w, lower, planes - 1 - s), upper, s)

    out_toks = gathered.shape[3] * CORES
    columns = w_out.shape[1]
    steps = 8
    out = pl.pallas_call(
        functools.partial(project, chips, planes, toks, steps),
        out_shape=jax.ShapeDtypeStruct((columns, out_toks), jnp.bfloat16),
        in_specs=[hbm, hbm],
        out_specs=vmem,
        scratch_shapes=[
            pltpu.VMEM((chips, planes, out_toks, v_dim), jnp.bfloat16),
            pltpu.VMEM((steps, planes, columns, chips // steps * v_dim), jnp.bfloat16),
            pltpu.SemaphoreType.DMA((steps, 1 + out_toks // toks)),
        ],
    )(gathered, all_w)
    return out.T


def solution(mesh):
    in_specs = (
        P(("groups", "ctx"), "tp"),
        P(("groups", "ctx"), "tp"),
        P(("groups", "ctx"), None),
        P(("groups", "ctx"), None),
        P(("groups", "ctx")),
        P("tp", "ctx", None),
        P("tp", "ctx", None),
        P("tp", "ctx"),
    )
    out_specs = P(("groups", "tp"), "ctx")

    return jax.shard_map(on_device, mesh=mesh, in_specs=in_specs, out_specs=out_specs, check_vma=False)
```

```python
import functools

import jax
import jax.numpy as jnp
import numpy as np
from jax import lax
from jax.experimental import pallas as pl
from jax.experimental.pallas import tpu as pltpu
from jax.sharding import PartitionSpec as P


LANES = 128
DIGIT = 32
CORES = 2


def frequencies(half_dim):
    return np.power(10000.0, -np.arange(half_dim) / half_dim).astype(np.float32)


def rotate(values, cosine, sine):
    half_dim = values.shape[-1] // 2
    first_half = values[..., :half_dim].astype(jnp.float32)
    second_half = values[..., half_dim:].astype(jnp.float32)
    return jnp.concatenate(
        [first_half * cosine - second_half * sine, second_half * cosine + first_half * sine],
        axis=-1,
    )


def prepare(chips, share, plane_ref, positions_ref, freqs_ref, c_kv_ref, k_rope_ref, out_ref):
    at = pl.multiple_of(plane_ref[0] * share, share)
    position = positions_ref[at] + lax.broadcasted_iota(jnp.int32, (share, 1), 0)
    angles = position.astype(jnp.float32) * freqs_ref[...]
    rotated = rotate(k_rope_ref[pl.ds(at, share), :], jnp.cos(angles), jnp.sin(angles))
    lane = lax.broadcasted_iota(jnp.int32, (share, LANES - rotated.shape[1]), 1)
    digits = jnp.where(lane == 0, position // DIGIT, jnp.where(lane == 1, position % DIGIT, 0))
    row = jnp.concatenate([rotated, digits.astype(jnp.float32)], axis=1).astype(jnp.bfloat16)
    row = jnp.concatenate([c_kv_ref[pl.ds(at, share), :], row], axis=1)
    for z in range(chips):
        out_ref[z] = row


def attend(chips, planes, toks, lat, scale, block, core_ref, q_ref, wv_ref, keys_ref, out_ref, pos_buf):
    share = toks // planes
    half = LANES // 2
    lane = lax.broadcasted_iota(jnp.int32, (LANES, LANES), 1)
    pick = jnp.where(lane == half, float(DIGIT), jnp.where(lane == half + 1, 1.0, 0.0))
    pick = pick.astype(jnp.bfloat16)
    nt = (((1,), (1,)), ((), ()))
    all_keys = keys_ref[...].reshape(CORES * chips * toks, lat + LANES)
    key_pos = lax.dot_general(pick[0:8], all_keys[:, lat:], nt, preferred_element_type=jnp.float32)[0:1]
    own = keys_ref[pl.ds(core_ref[0], 1), :, lat:].reshape(chips * toks, LANES)
    own_pos = lax.dot_general(own, pick, nt, preferred_element_type=jnp.float32)
    own_pos = own_pos.reshape(planes, chips, share, LANES)
    for x in range(planes):
        pos_buf[:, x] = own_pos[x]
    q_pos = pos_buf[...].reshape(chips * toks, LANES)[:, 0:1]
    factor = scale * 1.4426950408889634
    blocks = [slice(at, at + block) for at in range(0, chips * toks, block)]

    def score(rows):
        return lax.dot_general(q_ref[rows, :], all_keys, nt, preferred_element_type=jnp.float32)

    following = score(blocks[0])
    for b, rows in enumerate(blocks):
        scores = jnp.where(key_pos <= q_pos[rows], following, -1e30)
        if b + 1 < len(blocks):
            following = score(blocks[b + 1])
        top = jnp.max(scores, axis=1, keepdims=True)
        weights = jnp.exp2((scores - top) * factor)
        total = jnp.sum(weights, axis=1, keepdims=True)
        mixed = jnp.dot(
            weights.astype(jnp.bfloat16), all_keys[:, :lat], preferred_element_type=jnp.float32
        )
        o_lat = (mixed * (1.0 / total)).astype(jnp.bfloat16)
        out_ref[rows, :] = jnp.dot(
            o_lat, wv_ref[...], preferred_element_type=jnp.float32
        ).astype(jnp.bfloat16)


def project(chips, planes, toks, steps, gathered, weights, out_ref, heads_buf, w_buf, sems):
    each = chips // steps
    pairs = heads_buf.shape[2] // (CORES * toks)
    v_dim = heads_buf.shape[3]
    copies = []
    for s in range(steps):
        zs = slice(s * each, (s + 1) * each)
        group = [
            pltpu.make_async_copy(
                weights.at[:, :, s * each * v_dim : (s + 1) * each * v_dim], w_buf.at[s], sems.at[s, 0]
            )
        ]
        for pair in range(pairs):
            for k in range(CORES):
                at = (pair * CORES + k) * toks
                group.append(
                    pltpu.make_async_copy(
                        gathered.at[zs, k, :, pair * toks : (pair + 1) * toks, :],
                        heads_buf.at[zs, :, at : at + toks, :],
                        sems.at[s, 1 + pair * CORES + k],
                    )
                )
        copies.append(group)
    for group in copies:
        for c in group:
            c.start()
    total = None
    for s in range(steps):
        for c in copies[s]:
            c.wait()
        for i in range(each):
            z = s * each + i
            rows = jnp.concatenate([heads_buf[z, x] for x in range(planes)], axis=1)
            w = jnp.concatenate(
                [w_buf[s, x, :, i * v_dim : (i + 1) * v_dim] for x in range(planes)], axis=1
            )
            added = lax.dot_general(
                w, rows, (((1,), (1,)), ((), ())), preferred_element_type=jnp.float32
            )
            total = added if total is None else total + added
    out_ref[...] = total.astype(jnp.bfloat16)


def on_device(q_nope, q_rope, c_kv, k_rope, positions, w_uk, w_uv, w_out):
    toks, lat = c_kv.shape
    heads, tile_rows, _ = w_uk.shape
    ranks = lax.axis_size("ctx")
    planes = lax.axis_size("tp")
    chips = ranks // CORES
    assert heads == chips
    nope = tile_rows * ranks
    rope = k_rope.shape[1]
    v_rows, v_dim = w_uv.shape[1:]
    scale = (nope + rope) ** (-0.5)
    same_core = [[z * CORES + k for z in range(chips)] for k in range(CORES)]
    one_chip = [[z * CORES + k for k in range(CORES)] for z in range(chips)]

    plane = lax.axis_index("tp")
    share = toks // planes

    assert DIGIT % share == 0
    vmem = pl.BlockSpec(memory_space=pltpu.VMEM)
    smem = pl.BlockSpec(memory_space=pltpu.SMEM)
    freqs = jnp.asarray(frequencies(rope // 2))[None]
    own_keys = pl.pallas_call(
        functools.partial(prepare, chips, share),
        out_shape=jax.ShapeDtypeStruct((chips, share, lat + LANES), jnp.bfloat16),
        in_specs=[smem, smem, vmem, vmem, vmem],
        out_specs=vmem,
    )(plane.astype(jnp.int32).reshape(1), positions, freqs, c_kv, k_rope)
    own_keys = lax.all_to_all(
        own_keys, "ctx", split_axis=0, concat_axis=0, tiled=True, axis_index_groups=same_core
    )
    one_row = [[r * planes + x for r in range(z * CORES, (z + 1) * CORES) for x in range(planes)] for z in range(chips)]
    keys = lax.all_gather(
        own_keys.reshape(chips * share, -1),
        ("ctx", "tp"),
        axis=0,
        tiled=True,
        axis_index_groups=one_row,
    ).reshape(CORES, chips * toks, -1)

    angles = positions.astype(jnp.float32)[:, None] * freqs
    cosine, sine = jnp.cos(angles), jnp.sin(angles)
    q_parts = q_nope.reshape(toks, heads, nope).transpose(1, 0, 2)
    q_rot = rotate(q_rope.reshape(toks, heads, rope), cosine[:, None], sine[:, None])
    q_rot = q_rot.astype(jnp.bfloat16).transpose(1, 0, 2)
    q_rot = jnp.concatenate([q_rot[:, : toks // 2], q_rot[:, toks // 2 :]], axis=2)
    k_rows = tile_rows * lat // LANES
    sent = jnp.concatenate([q_parts, q_rot, w_uk.reshape(heads, k_rows, LANES), w_uv], axis=1)
    came = lax.all_to_all(
        sent, "ctx", split_axis=0, concat_axis=0, tiled=True, axis_index_groups=same_core
    )
    cut = toks + toks // 2
    q_parts = came[:, :toks].reshape(chips * toks, nope)
    q_rot = came[:, toks:cut]
    q_rot = jnp.concatenate([q_rot[:, :, :rope], q_rot[:, :, rope:]], axis=1).reshape(-1, rope)
    both = jnp.broadcast_to(came[None, :, cut:], (CORES, chips, k_rows + v_rows, LANES))
    both = lax.all_to_all(
        both, "ctx", split_axis=0, concat_axis=0, tiled=True, axis_index_groups=one_chip
    )
    both = both.transpose(1, 0, 2, 3)
    up_key = both[:, :, :k_rows].reshape(nope, lat)
    up_value = both[:, :, k_rows:].reshape(lat, v_dim)
    q_lat = jnp.dot(q_parts, up_key, preferred_element_type=jnp.float32).astype(jnp.bfloat16)
    queries = jnp.concatenate(
        [q_lat, q_rot, jnp.zeros((chips * toks, LANES - rope), jnp.bfloat16)], axis=1
    )

    own_w = w_out.T
    right = [(i, (i + 1) % planes) for i in range(planes)]
    left = [(i, (i - 1) % planes) for i in range(planes)]
    all_w = jnp.zeros((planes, *own_w.shape), jnp.bfloat16)

    def placed(stack, block, shift):
        return lax.dynamic_update_slice(stack, block[None], ((plane + shift) % planes, 0, 0))

    lower = lax.ppermute(own_w, "tp", right)
    all_w = placed(placed(all_w, own_w, 0), lower, planes - 1)
    upper = own_w

    hbm = pl.BlockSpec(memory_space=pl.ANY)
    core = (lax.axis_index("ctx") % CORES).astype(jnp.int32).reshape(1)
    block = min(256, chips * toks)
    head_out = pl.pallas_call(
        functools.partial(attend, chips, planes, toks, lat, scale, block),
        out_shape=jax.ShapeDtypeStruct((chips * toks, v_dim), jnp.bfloat16),
        in_specs=[smem, vmem, vmem, vmem],
        out_specs=vmem,
        scratch_shapes=[pltpu.VMEM((chips, planes, share, LANES), jnp.float32)],
        compiler_params=pltpu.CompilerParams(vmem_limit_bytes=20 * 2**20),
    )(core, queries, up_value, keys)

    by_plane = lax.all_to_all(
        head_out.reshape(planes, -1, v_dim), "tp", split_axis=0, concat_axis=0, tiled=True
    )
    gathered = lax.all_gather(by_plane.reshape(-1, v_dim), "ctx", axis=0)
    gathered = gathered.reshape(chips, CORES, planes, -1, v_dim)
    for s in range(1, planes // 2):
        lower = lax.ppermute(lower, "tp", right)
        upper = lax.ppermute(upper, "tp", left)
        all_w = placed(placed(all_w, lower, planes - 1 - s), upper, s)

    out_toks = gathered.shape[3] * CORES
    columns = w_out.shape[1]
    steps = 8
    out = pl.pallas_call(
        functools.partial(project, chips, planes, toks, steps),
        out_shape=jax.ShapeDtypeStruct((columns, out_toks), jnp.bfloat16),
        in_specs=[hbm, hbm],
        out_specs=vmem,
        scratch_shapes=[
            pltpu.VMEM((chips, planes, out_toks, v_dim), jnp.bfloat16),
            pltpu.VMEM((steps, planes, columns, chips // steps * v_dim), jnp.bfloat16),
            pltpu.SemaphoreType.DMA((steps, 1 + out_toks // toks)),
        ],
    )(gathered, all_w)
    return out.T


def solution(mesh):
    in_specs = (
        P(("groups", "ctx"), "tp"),
        P(("groups", "ctx"), "tp"),
        P(("groups", "ctx"), None),
        P(("groups", "ctx"), None),
        P(("groups", "ctx")),
        P("tp", "ctx", None),
        P("tp", "ctx", None),
        P("tp", "ctx"),
    )
    out_specs = P(("groups", "tp"), "ctx")

    return jax.shard_map(on_device, mesh=mesh, in_specs=in_specs, out_specs=out_specs, check_vma=False)
```
